256 devices in a mesh: seqa: 16 (over x_hi, z), seqb: 16 (over x_lo, y, core).
Axes of the slice: x: 4 (x_hi: 2, x_lo: 2; x = x_hi * 2 + x_lo), y: 4, z: 8, core: 2. Of those that a mesh axis runs over, the one named last changes fastest.
Arguments:
- queries: bfloat16 [131072, 4096], P(('seqa', 'seqb')), may hold values from -60 to 60
- keys: bfloat16 [131072, 1024], P(('seqa', 'seqb')), may hold values from -8 to 8
- values: bfloat16 [131072, 1024], P(('seqa', 'seqb')), may hold values from -6 to 6
- doc_start: int32 [131072], P(('seqa', 'seqb')), may hold values from 0 to 131071, as said below
Outputs:
- attended: bfloat16 [131072, 4096], P(('seqa', 'seqb'))
The draws below stay inside these ranges and needn't reach their ends.
Inputs may be any that keep to these rules, and one draw needn't show every extreme that they name: Never falling along the sequence, doc_start[i] <= i, the same value for all tokens of one document, and doc_start[0] = 0.
All inputs are finite; a program needn't handle non-finite values.
Results may differ from the reference program's by a relative error of at most 0.0038.
Values may be sent and summed in bfloat16 or wider, within the bound.
A program may use at most 64 MiB of HBM per device.

```python
import math
import jax
import jax.numpy as jnp
from jax import lax

QUERY_HEADS = 32
KEY_VALUE_HEADS = 8
HEAD_SIZE = 128
TOK_DEV = 512
SEQUENCE_TOKENS = 131072


def query_key_pair(key):
    base = jax.random.fold_in(key, 11)
    query_key, key_random_seed = jax.random.split(base, 2)
    sampled_keys = jax.random.truncated_normal(key_random_seed, -6.0, 6.0, (SEQUENCE_TOKENS, KEY_VALUE_HEADS * HEAD_SIZE), jnp.float32)
    queries_drawn = jax.random.truncated_normal(query_key, -6.0, 6.0, (SEQUENCE_TOKENS, QUERY_HEADS * HEAD_SIZE), jnp.float32)
    return (queries_drawn, sampled_keys)


def draw_queries(key, part):
    return query_key_pair(key)[0].astype(jnp.bfloat16)


def draw_keys(key, part):
    return query_key_pair(key)[1].astype(jnp.bfloat16)


def draw_doc_start(key, part):
    marks = jax.random.randint(jax.random.fold_in(key, 3), (SEQUENCE_TOKENS,), 0, 2 * TOK_DEV)
    places = jnp.arange(SEQUENCE_TOKENS, dtype=jnp.int32)
    opening = (marks == 0) & (places >= 3 * TOK_DEV) | (places == 0)
    begins = jnp.where(opening, places, 0).astype(jnp.int32)
    return lax.cummax(begins, axis=0)


def shard_levels(own_key, shape, cuts, smallest, largest):
    def one(axis_at, parts):
        heights = jax.random.uniform(jax.random.fold_in(jax.random.fold_in(own_key, 6), axis_at), (parts,), jnp.float32, smallest / len(cuts), largest / len(cuts))
        return jnp.repeat(jnp.exp(heights), shape[axis_at] // parts).reshape((-1,) + (1,) * (len(shape) - axis_at - 1))

    gain = one(*cuts[0])
    for cut in cuts[1:]:
        gain = gain * one(*cut)
    return gain


def scatter_about(rng, shape, width, limit, shards=(), kind=jnp.bfloat16):
    loudness = shard_levels(rng, shape, shards, -0.22, 0.18) if shards else 1.0
    values = jax.random.normal(rng, shape, jnp.float32) * width * loudness
    return jnp.minimum(jnp.maximum(values, -limit), limit).astype(kind)


def setup_inputs(seed: int = 0) -> dict:
    arg_keys = jax.random.split(jax.random.key(seed), 5)
    queries = draw_queries(jax.random.fold_in(arg_keys[4], 71), 0)
    keys = draw_keys(jax.random.fold_in(arg_keys[4], 71), 0)
    values = scatter_about(arg_keys[2], (SEQUENCE_TOKENS, KEY_VALUE_HEADS * HEAD_SIZE), 1.0, 6.0, ((0, 256),))
    doc_start = draw_doc_start(jax.random.fold_in(arg_keys[4], 71), 0)
    return {"queries": queries, "keys": keys, "values": values, "doc_start": doc_start}


def reference(queries, keys, values, doc_start):
    rows_per_block = min(512, TOK_DEV)
    window_length = 2 * TOK_DEV
    group_width = QUERY_HEADS // KEY_VALUE_HEADS
    score_scale = 1.0 / math.sqrt(HEAD_SIZE)
    padded_keys = jnp.concatenate([jnp.zeros((window_length, KEY_VALUE_HEADS * HEAD_SIZE), jnp.bfloat16), keys], axis=0)
    padded_values = jnp.concatenate([jnp.zeros((window_length, KEY_VALUE_HEADS * HEAD_SIZE), jnp.bfloat16), values], axis=0)

    def one_block(block_index):
        offset = (block_index * rows_per_block).astype(jnp.int32)
        block_of_queries = lax.dynamic_slice_in_dim(queries, offset, rows_per_block, 0).astype(jnp.float32)
        block_of_queries = block_of_queries.reshape(rows_per_block, KEY_VALUE_HEADS, group_width, HEAD_SIZE)
        block_of_keys = lax.dynamic_slice_in_dim(padded_keys, offset, window_length + rows_per_block, 0).astype(jnp.float32)
        block_of_keys = block_of_keys.reshape(window_length + rows_per_block, KEY_VALUE_HEADS, HEAD_SIZE)
        block_of_values = lax.dynamic_slice_in_dim(padded_values, offset, window_length + rows_per_block, 0).astype(jnp.float32)
        block_of_values = block_of_values.reshape(window_length + rows_per_block, KEY_VALUE_HEADS, HEAD_SIZE)
        scores = jnp.einsum('thgd,khd->hgtk', block_of_queries, block_of_keys) * score_scale
        query_place = offset + jnp.arange(rows_per_block, dtype=jnp.int32)
        key_place = offset - window_length + jnp.arange(window_length + rows_per_block, dtype=jnp.int32)
        starts = lax.dynamic_slice_in_dim(doc_start, offset, rows_per_block, 0)
        visible = (key_place[None, :] <= query_place[:, None]) & (key_place[None, :] > query_place[:, None] - window_length) & (key_place[None, :] >= starts[:, None])
        scores = jnp.where(visible[None, None], scores, jnp.float32(-1e+30))
        row_top = lax.optimization_barrier(jnp.max(scores, axis=-1, keepdims=True))
        exponent = jnp.where(visible[None, None], jnp.exp(scores - row_top), jnp.float32(0.0))
        row_sum = lax.optimization_barrier(jnp.sum(exponent, axis=-1, keepdims=True))
        weights = exponent.astype(jnp.bfloat16).astype(jnp.float32)
        summed = jnp.einsum('hgtk,khd->thgd', weights, block_of_values)
        result = summed / jnp.transpose(row_sum, (2, 0, 1, 3))
        return result.reshape(rows_per_block, QUERY_HEADS * HEAD_SIZE).astype(jnp.bfloat16)
    blocks = lax.map(one_block, jnp.arange(SEQUENCE_TOKENS // rows_per_block, dtype=jnp.int32))
    return blocks.reshape(SEQUENCE_TOKENS, QUERY_HEADS * HEAD_SIZE)
```

```python
import functools
import math

import jax
import jax.numpy as jnp
from jax import lax
from jax.experimental import pallas as pl
from jax.experimental.pallas import tpu as pltpu
from jax.sharding import PartitionSpec as P

MESH = pl.DeviceIdType.MESH
HEAD = 128
ROWS = 512
BLOCK = 256
SPAN = 5 * BLOCK
SCALE = math.log2(math.e) / math.sqrt(HEAD)
ROUND = (4, 7)
COLUMN = 4


def places(chips):
    seqb = lax.axis_index("seqb")
    wide = lax.axis_size("seqb") // 2
    chip = lax.axis_index("seqa") * wide + seqb // 2
    core = lax.rem(seqb, 2)
    y = lax.rem(chip, COLUMN)

    def at(chip_index, core_index=core):
        return (chip_index // wide, lax.rem(chip_index, wide) * 2 + core_index)

    def in_column(chip_index, step):
        place = lax.rem(chip_index, COLUMN)
        return chip_index - place + lax.rem(place + step, COLUMN)

    before = lax.rem(chip + chips - 1, chips)
    return dict(
        core=core,
        partner=at(chip, 1 - core),
        after=at(lax.rem(chip + 1, chips)),
        before=at(before),
        down=at(in_column(chip, 3)),
        up=at(in_column(chip, 1)),
        last_to=at(lax.rem(in_column(chip, 2) + 1, chips)),
        last_from=at(in_column(before, 2)),
    )


def attend(head, q_ref, kv, bias, scores, weights, out, block):
    rows = slice(block * BLOCK, (block + 1) * BLOCK)
    keys = block * BLOCK
    for g in range(4):
        unit = (block * 4 + g) % 2
        s_ref, w_ref = scores.at[unit], weights.at[unit]
        columns = pl.ds(pl.multiple_of(head * 4 * HEAD, 4 * HEAD) + g * HEAD, HEAD)
        q = q_ref[rows, columns]
        top = None
        for t in range(5):
            span = slice(t * BLOCK, (t + 1) * BLOCK)
            k = kv[head, 0, keys + t * BLOCK : keys + (t + 1) * BLOCK, :]
            s = lax.dot_general(
                q, k, (((1,), (1,)), ((), ())), preferred_element_type=jnp.float32
            )
            s = jnp.minimum(s, bias[block, :, span])
            s_ref[:, span] = s
            s = jnp.maximum(s[:, :HEAD], s[:, HEAD:])
            top = s if top is None else jnp.maximum(top, s)
        top = jnp.max(top, axis=1, keepdims=True)
        for t in range(5):
            span = slice(t * BLOCK, (t + 1) * BLOCK)
            w = jnp.exp2((s_ref[:, span] - top) * SCALE)
            w_ref[:, span] = w.astype(jnp.bfloat16)
        v = kv[head, 1, keys : keys + SPAN, :]
        v = jnp.concatenate([v, jnp.ones((SPAN, HEAD), jnp.bfloat16)], axis=1)
        o = jnp.dot(w_ref[...], v, preferred_element_type=jnp.float32)
        o = o[:, :HEAD] / o[:, HEAD:]
        out[rows, columns] = o.astype(jnp.bfloat16)


def kernel(
    chips, q_hbm, k_hbm, v_hbm, start_ref, o_hbm,
    q_ref, kv, hop, bias, scores, weights, out,
    kv_sem, q_sem, o_sem, far_send, far_recv, near_send, near_recv, hop_send, hop_recv,
):
    heads = kv.shape[0]
    at = places(chips)
    own, one, two = slice(1024, 1536), slice(512, 1024), slice(0, 512)

    def load_kv(h, which):
        src = (k_hbm, v_hbm)[which]
        return pltpu.make_async_copy(
            src.at[:, pl.ds(h * HEAD, HEAD)], kv.at[h, which, own], kv_sem.at[h, which]
        )

    def load_q(h):
        columns = pl.ds(pl.multiple_of(h * 4 * HEAD, 4 * HEAD), 4 * HEAD)
        return pltpu.make_async_copy(q_hbm.at[:, columns], q_ref.at[:, columns], q_sem.at[h])

    def store_o(h):
        columns = pl.ds(pl.multiple_of(h * 4 * HEAD, 4 * HEAD), 4 * HEAD)
        return pltpu.make_async_copy(out.at[:, columns], o_hbm.at[:, columns], o_sem.at[h])

    def far(h):
        return pltpu.make_async_remote_copy(
            kv.at[h, :, own], kv.at[h, :, two], far_send.at[h], far_recv.at[h],
            device_id=at["after"], device_id_type=MESH,
        )

    def near(h, src):
        return pltpu.make_async_remote_copy(
            kv.at[h, :, src], kv.at[h, :, one], near_send.at[h], near_recv.at[h],
            device_id=at["partner"], device_id_type=MESH,
        )

    def first_hop(i):
        return pltpu.make_async_remote_copy(
            kv.at[ROUND[i], :, own], hop.at[0, i], hop_send.at[0, i], hop_recv.at[0, i],
            device_id=at["down"], device_id_type=MESH,
        )

    def second_hop(i):
        return pltpu.make_async_remote_copy(
            hop.at[0, i], hop.at[1, i], hop_send.at[1, i], hop_recv.at[1, i],
            device_id=at["down"], device_id_type=MESH,
        )

    def third_hop(i):
        h = ROUND[i]
        return pltpu.make_async_remote_copy(
            hop.at[1, i], kv.at[h, :, two], far_send.at[h], far_recv.at[h],
            device_id=at["last_to"], device_id_type=MESH,
        )

    order = [0, ROUND[0]] + [h for h in range(1, heads) if h not in (ROUND[0],)]
    for h in order:
        for which in range(2):
            load_kv(h, which).start()
    for h in range(heads):
        load_q(h).start()

    barrier = pltpu.get_barrier_semaphore()
    peers = ("partner", "after", "before", "down", "up", "last_to", "last_from")
    for name in peers:
        pl.semaphore_signal(barrier, inc=1, device_id=at[name], device_id_type=MESH)

    shard = lax.axis_index("seqa") * lax.axis_size("seqb") + lax.axis_index("seqb")
    for block in range(2):
        starts = []
        for r in range(2):
            row = start_ref[pl.ds(block * 2 + r, 1), :] - shard * ROWS
            row = jnp.broadcast_to(row.astype(jnp.float32), (HEAD, HEAD))
            starts.append(row.T)
        start = jnp.concatenate(starts, axis=0)
        for t in range(SPAN // HEAD):
            q_place = lax.broadcasted_iota(jnp.int32, (BLOCK, HEAD), 0) + block * BLOCK
            k_place = lax.broadcasted_iota(jnp.int32, (BLOCK, HEAD), 1) + (
                t * HEAD + block * BLOCK - 2 * ROWS
            )
            seen = (
                (k_place <= q_place)
                & (k_place > q_place - 2 * ROWS)
                & (k_place.astype(jnp.float32) >= start)
            )
            bias[block, :, t * HEAD : (t + 1) * HEAD] = jnp.where(
                seen, jnp.float32(3e38), jnp.float32(-1e30)
            )

    pl.semaphore_wait(barrier, len(peers))

    for h in order:
        for which in range(2):
            load_kv(h, which).wait()
        if h in ROUND:
            first_hop(ROUND.index(h)).start()
        else:
            far(h).start()

        @pl.when(at["core"] == 0)
        def _():
            near(h, own).start()

    def step(h, carry):
        for i in range(2):

            @pl.when(h == i)
            def _():
                first_hop(i).wait_recv()
                second_hop(i).start()

            @pl.when(h == 2 + i)
            def _():
                second_hop(i).wait_recv()
                third_hop(i).start()

        far(h).wait_recv()

        @pl.when(at["core"] == 1)
        def _():
            near(h, two).start()

        load_q(h).wait()
        near(h, own).wait_recv()
        for block in range(2):
            attend(h, q_ref, kv, bias, scores, weights, out, block)
        store_o(h).start()
        return carry

    lax.fori_loop(0, heads, step, 0)

    for h in range(heads):
        store_o(h).wait()
        near(h, own).wait_send()
        if h not in ROUND:
            far(h).wait_send()
    for i in range(2):
        first_hop(i).wait_send()
        second_hop(i).wait_send()
        third_hop(i).wait_send()


def local(queries, keys, values, doc_start):
    heads = keys.shape[1] // HEAD
    chips = lax.axis_size("seqa") * lax.axis_size("seqb") // 2
    anywhere = pl.BlockSpec(memory_space=pl.ANY)
    dma = pltpu.SemaphoreType.DMA
    return pl.pallas_call(
        functools.partial(kernel, chips),
        out_shape=jax.ShapeDtypeStruct(queries.shape, queries.dtype),
        in_specs=[anywhere] * 3 + [pl.BlockSpec(memory_space=pltpu.VMEM)],
        out_specs=anywhere,
        scratch_shapes=[
            pltpu.VMEM(queries.shape, jnp.bfloat16),
            pltpu.VMEM((heads, 2, 3 * ROWS, HEAD), jnp.bfloat16),
            pltpu.VMEM((2, 2, 2, ROWS, HEAD), jnp.bfloat16),
            pltpu.VMEM((2, BLOCK, SPAN), jnp.float32),
            pltpu.VMEM((2, BLOCK, SPAN), jnp.float32),
            pltpu.VMEM((2, BLOCK, SPAN), jnp.bfloat16),
            pltpu.VMEM(queries.shape, jnp.bfloat16),
            dma((heads, 2)), dma((heads,)), dma((heads,)),
            dma((heads,)), dma((heads,)), dma((heads,)), dma((heads,)),
            dma((2, 2)), dma((2, 2)),
        ],
        compiler_params=pltpu.CompilerParams(
            collective_id=0, has_side_effects=True, vmem_limit_bytes=60 * 2**20
        ),
        name="attention",
    )(queries, keys, values, doc_start.reshape(ROWS // HEAD, HEAD))


def solution(mesh):
    shards = P(("seqa", "seqb"), None)
    return jax.shard_map(
        local,
        mesh=mesh,
        in_specs=(shards, shards, shards, P(("seqa", "seqb"))),
        out_specs=shards,
        check_vma=False,
    )
```

```python
import functools
import math

import jax
import jax.numpy as jnp
from jax import lax
from jax.experimental import pallas as pl
from jax.experimental.pallas import tpu as pltpu
from jax.sharding import PartitionSpec as P

MESH = pl.DeviceIdType.MESH
HEAD = 128
ROWS = 512
BLOCK = 256
SPAN = 5 * BLOCK
SCALE = math.log2(math.e) / math.sqrt(HEAD)
ROUND = ((4, 0), (4, 1), (7, 0))
LAST = 7
COLUMN = 4


def places(chips):
    seqb = lax.axis_index("seqb")
    wide = lax.axis_size("seqb") // 2
    chip = lax.axis_index("seqa") * wide + seqb // 2
    core = lax.rem(seqb, 2)

    def at(chip_index, core_index=core):
        return (chip_index // wide, lax.rem(chip_index, wide) * 2 + core_index)

    def in_column(chip_index, step):
        place = lax.rem(chip_index, COLUMN)
        return chip_index - place + lax.rem(place + step, COLUMN)

    before = lax.rem(chip + chips - 1, chips)
    return dict(
        core=core,
        partner=at(chip, 1 - core),
        after=at(lax.rem(chip + 1, chips)),
        before=at(before),
        down=at(in_column(chip, 3)),
        up=at(in_column(chip, 1)),
        last_to=at(lax.rem(in_column(chip, 2) + 1, chips)),
        last_from=at(in_column(before, 2)),
        has_before=chip != 0,
        peers=4 - (chip + 1) // chips - (in_column(chip, 2) + 1) // chips,
        has_after=chip != chips - 1,
        has_last_to=in_column(chip, 2) != chips - 1,
    )


def scaled(x):
    return jnp.exp2(x * SCALE)


def attend(head, slot, q_ref, kv, bias, scores, weights, state, out, blocks, part, between=None):
    units = [(block, g) for block in blocks for g in range(4)]
    tops = {}

    def span_of(block):
        first = 2 * ROWS if part == "own" else block * BLOCK
        last = 2 * ROWS if part == "before" else block * BLOCK + SPAN
        return first, last, range(first, last, BLOCK)

    def place(block, g):
        columns = pl.ds(slot * 4 * HEAD + g * HEAD, HEAD)
        return slice(block * BLOCK, (block + 1) * BLOCK), columns

    def score(n, x):
        block, g = units[n]
        first, last, _ = span_of(block)
        span, seen = (slice(x - y, x - y + BLOCK) for y in (first, block * BLOCK))
        k = kv[slot, 0, x : x + BLOCK, :]
        s = lax.dot_general(
            q_ref[place(block, g)], k, (((1,), (1,)), ((), ())), preferred_element_type=jnp.float32
        )
        s = jnp.minimum(s, bias[block, :, seen])
        scores[n % 2, :, span] = s
        s = jnp.maximum(s[:, :HEAD], s[:, HEAD:])
        if x > first:
            s = jnp.maximum(s, tops[n])
        elif part == "before":
            s = jnp.maximum(s, state[2][head, block * 4 + g])
        tops[n] = jnp.max(s, axis=1, keepdims=True) if x + BLOCK == last else s

    def weigh(n, x):
        span = slice(x - span_of(units[n][0])[0], x - span_of(units[n][0])[0] + BLOCK)
        weights[n % 2, :, span] = scaled(scores[n % 2, :, span] - tops[n]).astype(jnp.bfloat16)

    def gather(n):
        block, g = units[n]
        unit = block * 4 + g
        first, last, _ = span_of(block)
        v = kv[slot, 1, first:last, :]
        v = jnp.concatenate([v, jnp.ones((last - first, HEAD), jnp.bfloat16)], axis=1)
        o = jnp.dot(weights[n % 2, :, : last - first], v, preferred_element_type=jnp.float32)
        o, total = o[:, :HEAD], o[:, HEAD:]
        if part == "own":
            state[0][head, unit] = o
            state[1][head, unit] = total
            state[2][head, unit] = jnp.broadcast_to(tops[n], (BLOCK, HEAD))
            return
        if part == "before":
            fade = scaled(state[2][head, unit] - tops[n])
            o += fade * state[0][head, unit]
            total += fade * state[1][head, unit]
        out[place(block, g)] = (o / total).astype(jnp.bfloat16)

    for x in span_of(units[0][0])[2]:
        score(0, x)
    for n in range(len(units)):
        now = list(span_of(units[n][0])[2])
        later = list(span_of(units[n + 1][0])[2]) if n + 1 < len(units) else []
        for i in range(max(len(now), len(later))):
            if i < len(later):
                score(n + 1, later[i])
            if i < len(now):
                weigh(n, now[i])
        gather(n)
        if n == 3 and between:
            between()


def fill_bias(start_ref, bias):
    shard = lax.axis_index("seqa") * lax.axis_size("seqb") + lax.axis_index("seqb")
    for block in range(2):
        starts = []
        for r in range(2):
            row = start_ref[pl.ds(block * 2 + r, 1), :] - shard * ROWS
            row = jnp.broadcast_to(row.astype(jnp.float32), (HEAD, HEAD))
            starts.append(row.T)
        start = jnp.concatenate(starts, axis=0)
        for t in range(SPAN // HEAD):
            q_place = lax.broadcasted_iota(jnp.int32, (BLOCK, HEAD), 0) + block * BLOCK
            k_place = lax.broadcasted_iota(jnp.int32, (BLOCK, HEAD), 1) + (
                t * HEAD + block * BLOCK - 2 * ROWS
            )
            seen = (
                (k_place <= q_place)
                & (k_place > q_place - 2 * ROWS)
                & (k_place.astype(jnp.float32) >= start)
            )
            bias[block, :, t * HEAD : (t + 1) * HEAD] = jnp.where(
                seen, jnp.float32(3e38), jnp.float32(-1e30)
            )


def head_columns(h):
    return pl.ds(pl.multiple_of(h * 4 * HEAD, 4 * HEAD), 4 * HEAD)


def kernel(
    chips, q_hbm, k_hbm, v_hbm, start_ref, o_hbm, kv_last,
    q_ref, kv, hop, bias, scores, weights, acc, total, top, out,
    kv_sem, q_sem, o_sem, pad_sem, far_send, far_recv, near_send, near_recv,
    hop_send, hop_recv,
):
    heads = kv.shape[0]
    at = places(chips)
    own, one, two = slice(1024, 1536), slice(512, 1024), slice(0, 512)
    rounds = range(len(ROUND))
    late = [i for i in rounds if ROUND[i][0] == LAST]
    early = [i for i in rounds if ROUND[i][0] != LAST]
    (lone,) = {ROUND[i][0] for i in early}

    def load_kv(h, which):
        src = (k_hbm, v_hbm)[which]
        return pltpu.make_async_copy(
            src.at[:, pl.ds(h * HEAD, HEAD)], kv.at[h, which, own], kv_sem.at[h, which]
        )

    def load_q(h):
        columns = head_columns(h)
        return pltpu.make_async_copy(q_hbm.at[:, columns], q_ref.at[:, columns], q_sem.at[h])

    def store_o(h):
        columns = head_columns(h)
        return pltpu.make_async_copy(out.at[:, columns], o_hbm.at[:, columns], o_sem.at[h])

    def pad(h):
        dst = kv_last.at[:, two] if h is LAST else kv.at[h, :, two]
        return pltpu.make_async_copy(kv.at[h, :, own], dst, pad_sem.at[h])

    def sent(src, dst, sems, place):
        send, recv = sems
        return pltpu.make_async_remote_copy(
            src, dst, send, recv, device_id=at[place], device_id_type=MESH
        )

    def far(h):
        sems = far_send.at[h], far_recv.at[h]
        if h is LAST:
            return sent(kv.at[h, 1, own], kv_last.at[1, two], sems, "after")
        return sent(kv.at[h, :, own], kv.at[h, :, two], sems, "after")

    def near(h, src):
        sems = near_send.at[h], near_recv.at[h]
        if h is not LAST:
            return sent(kv.at[h, :, src], kv.at[h, :, one], sems, "partner")
        src = kv_last.at[:, src] if src is two else kv.at[h, :, src]
        return sent(src, kv_last.at[:, one], sems, "partner")

    def hops(stage, i):
        h, which = ROUND[i]
        sems = hop_send.at[stage, i], hop_recv.at[stage, i]
        if stage == 0:
            return sent(kv.at[h, which, own], hop.at[0, i], sems, "down")
        if stage == 1:
            return sent(hop.at[0, i], hop.at[1, i], sems, "down")
        dst = kv_last.at[which, two] if h is LAST else kv.at[h, which, two]
        return sent(hop.at[1, i], dst, sems, "last_to")

    def second(i):
        hops(0, i).wait_recv()
        hops(1, i).start()

    def third(i):
        hops(1, i).wait_recv()

        @pl.when(at["has_last_to"])
        def _():
            hops(2, i).start()

    order = [0, lone, LAST, *(h for h in range(1, LAST) if h != lone)]
    for h in order:
        for which in range(2):
            load_kv(h, which).start()
    for h in range(heads - 1):
        load_q(h).start()

    barrier = pltpu.get_barrier_semaphore()

    def ready(name):
        pl.semaphore_signal(barrier, inc=1, device_id=at[name], device_id_type=MESH)

    ready("partner")
    ready("up")

    @pl.when(at["has_before"])
    def _():
        ready("before")
        ready("last_from")

    pl.semaphore_wait(barrier, at["peers"])

    for h in order:
        for which in range(2):
            load_kv(h, which).wait()
        for i in rounds:
            if ROUND[i][0] == h:
                hops(0, i).start()

        @pl.when(at["has_after"])
        def _():
            if h not in (lone, LAST):
                far(h).start()

        @pl.when(at["core"] == 0)
        def _():
            near(h, own).start()

        @pl.when(jnp.logical_not(at["has_before"]))
        def _():
            pad(h).start()

    @pl.when(at["has_after"])
    def _():
        far(LAST).start()

    fill_bias(start_ref, bias)
    state = (acc, total, top)

    def first_step(h, carry):
        load_q(h).wait()
        attend(h, h, q_ref, kv, bias, scores, weights, state, out, (0, 1), "own")

        @pl.when(h == heads - 3)
        def _():
            second(0)
            second(1)

        return carry

    lax.fori_loop(0, heads - 1, first_step, 0)

    def step(h, carry):
        @pl.when(h == 0)
        def _():
            second(2)

        @pl.when(h == 2)
        def _():
            third(0)
            third(1)

        @pl.when(h == 3)
        def _():
            third(2)

        @pl.when(at["has_before"])
        def _():
            @pl.when(h != lone)
            def _():
                far(h).wait_recv()

            @pl.when(h == lone)
            def _():
                for i in early:
                    hops(2, i).wait_recv()

        @pl.when(jnp.logical_not(at["has_before"]))
        def _():
            pad(h).wait()

        @pl.when(at["core"] == 1)
        def _():
            near(h, two).start()

        near(h, own).wait_recv()
        work = q_ref, kv, bias, scores, weights, state, out
        if not isinstance(h, int):
            attend(h, h, *work, (0, 1), "before")
        else:
            attend(h, h, *work, (0,), "before")

            @pl.when(at["has_before"])
            def _():
                for i in late:
                    hops(2, i).wait_recv()
                far(LAST).wait_recv()

            @pl.when(jnp.logical_not(at["has_before"]))
            def _():
                pad(LAST).wait()

            @pl.when(at["core"] == 1)
            def _():
                near(LAST, two).start()

            attend(h, h, *work, (1,), "before")
        store_o(h).start()
        return carry

    lax.fori_loop(0, heads - 2, step, 0)
    step(heads - 2, 0)

    near(LAST, own).wait_recv()
    for h in range(heads):
        if h != LAST:
            store_o(h).wait()
        near(h, own).wait_send()
        if h != lone:

            @pl.when(at["has_after"])
            def _():
                far(h).wait_send()

    for i in rounds:
        hops(0, i).wait_send()
        hops(1, i).wait_send()

        @pl.when(at["has_last_to"])
        def _():
            hops(2, i).wait_send()


def finish(
    q_hbm, k_hbm, v_hbm, start_ref, first_hbm, kv_last, o_hbm,
    q_ref, kv, bias, scores, weights, out, kv_sem, q_sem, in_sem, o_sem,
):
    heads = k_hbm.shape[1] // HEAD
    columns = head_columns(LAST)
    loads = [
        pltpu.make_async_copy(kv_last, kv.at[0, :, : 2 * ROWS], kv_sem.at[0]),
        pltpu.make_async_copy(k_hbm.at[:, pl.ds(LAST * HEAD, HEAD)], kv.at[0, 0, 2 * ROWS :], kv_sem.at[1]),
        pltpu.make_async_copy(v_hbm.at[:, pl.ds(LAST * HEAD, HEAD)], kv.at[0, 1, 2 * ROWS :], kv_sem.at[2]),
        pltpu.make_async_copy(q_hbm.at[:, columns], q_ref, q_sem),
    ]
    takes = [
        pltpu.make_async_copy(first_hbm.at[:, head_columns(h)], out.at[h], in_sem.at[h])
        for h in range(heads - 1)
    ]
    stores = [
        pltpu.make_async_copy(out.at[h], o_hbm.at[:, head_columns(h)], o_sem.at[h])
        for h in range(heads - 1)
    ]
    halves = [
        pltpu.make_async_copy(
            out.at[LAST, pl.ds(block * BLOCK, BLOCK)],
            o_hbm.at[pl.ds(block * BLOCK, BLOCK), columns],
            o_sem.at[LAST + block],
        )
        for block in range(2)
    ]
    for copy in loads:
        copy.start()
    fill_bias(start_ref, bias)
    for copy in loads:
        copy.wait()
    for copy in takes:
        copy.start()

    def between():
        halves[0].start()
        for h in range(heads - 1):
            takes[h].wait()
            stores[h].start()

    attend(0, 0, q_ref, kv, bias, scores, weights, None, out.at[LAST], (0, 1), "all", between)
    halves[1].start()
    for copy in stores + halves:
        copy.wait()


def local(queries, keys, values, doc_start):
    heads = keys.shape[1] // HEAD
    chips = lax.axis_size("seqa") * lax.axis_size("seqb") // 2
    anywhere = pl.BlockSpec(memory_space=pl.ANY)
    held = pl.BlockSpec(memory_space=pltpu.VMEM)
    dma = pltpu.SemaphoreType.DMA
    starts = doc_start.reshape(ROWS // HEAD, HEAD)
    work = [
        pltpu.VMEM((2, BLOCK, SPAN), jnp.float32),
        pltpu.VMEM((2, BLOCK, SPAN), jnp.float32),
        pltpu.VMEM((2, BLOCK, SPAN), jnp.bfloat16),
    ]
    first, kv_last = pl.pallas_call(
        functools.partial(kernel, chips),
        out_shape=(
            jax.ShapeDtypeStruct(queries.shape, queries.dtype),
            jax.ShapeDtypeStruct((2, 2 * ROWS, HEAD), keys.dtype),
        ),
        in_specs=[anywhere] * 3 + [held],
        out_specs=(anywhere, anywhere),
        scratch_shapes=[
            pltpu.VMEM(queries.shape, jnp.bfloat16),
            pltpu.VMEM((heads, 2, 3 * ROWS, HEAD), jnp.bfloat16),
            pltpu.VMEM((2, len(ROUND), ROWS, HEAD), jnp.bfloat16),
            *work,
            *[pltpu.VMEM((heads - 1, 8, BLOCK, HEAD), jnp.float32)] * 3,
            pltpu.VMEM(queries.shape, jnp.bfloat16),
            dma((heads, 2)), dma((heads,)), dma((heads,)), dma((heads,)),
            dma((heads,)), dma((heads,)), dma((heads,)), dma((heads,)),
            dma((3, len(ROUND))), dma((3, len(ROUND))),
        ],
        compiler_params=pltpu.CompilerParams(
            collective_id=0, has_side_effects=True, vmem_limit_bytes=60 * 2**20
        ),
        name="attention",
    )(queries, keys, values, starts)
    return pl.pallas_call(
        finish,
        out_shape=jax.ShapeDtypeStruct(queries.shape, queries.dtype),
        in_specs=[anywhere] * 3 + [held] + [anywhere] * 2,
        out_specs=anywhere,
        scratch_shapes=[
            pltpu.VMEM((ROWS, 4 * HEAD), jnp.bfloat16),
            pltpu.VMEM((1, 2, 3 * ROWS, HEAD), jnp.bfloat16),
            *work,
            pltpu.VMEM((heads, ROWS, 4 * HEAD), jnp.bfloat16),
            dma((3,)), dma, dma((heads,)), dma((heads + 1,)),
        ],
        compiler_params=pltpu.CompilerParams(vmem_limit_bytes=60 * 2**20),
        name="finish",
    )(queries, keys, values, starts, first, kv_last)


def solution(mesh):
    shards = P(("seqa", "seqb"), None)
    return jax.shard_map(
        local,
        mesh=mesh,
        in_specs=(shards, shards, shards, P(("seqa", "seqb"))),
        out_specs=shards,
        check_vma=False,
    )
```

```python
import functools
import math

import jax
import jax.numpy as jnp
from jax import lax
from jax.experimental import pallas as pl
from jax.experimental.pallas import tpu as pltpu
from jax.sharding import PartitionSpec as P

MESH = pl.DeviceIdType.MESH
HEAD = 128
ROWS = 512
BLOCK = 256
SPAN = 5 * BLOCK
SCALE = math.log2(math.e) / math.sqrt(HEAD)
ROUND = ((4, 0, 512), (4, 1, 512), (6, 0, 512), (6, 1, 256))
SPLIT = 6
LAST = 7
COLUMN = 4


def places(chips):
    seqb = lax.axis_index("seqb")
    wide = lax.axis_size("seqb") // 2
    chip = lax.axis_index("seqa") * wide + seqb // 2
    core = lax.rem(seqb, 2)

    def at(chip_index, core_index=core):
        return (chip_index // wide, lax.rem(chip_index, wide) * 2 + core_index)

    def in_column(chip_index, step):
        place = lax.rem(chip_index, COLUMN)
        return chip_index - place + lax.rem(place + step, COLUMN)

    before = lax.rem(chip + chips - 1, chips)
    return dict(
        core=core,
        partner=at(chip, 1 - core),
        after=at(lax.rem(chip + 1, chips)),
        before=at(before),
        down=at(in_column(chip, 3)),
        up=at(in_column(chip, 1)),
        last_to=at(lax.rem(in_column(chip, 2) + 1, chips)),
        last_from=at(in_column(before, 2)),
        has_before=chip != 0,
        peers=4 - (chip + 1) // chips - (in_column(chip, 2) + 1) // chips,
        has_after=chip != chips - 1,
        has_last_to=in_column(chip, 2) != chips - 1,
    )


def scaled(x):
    return jnp.exp2(x * SCALE)


def attend(head, slot, q_ref, kv, bias, scores, weights, state, out, blocks, part, between=None):
    units = [(block, g) for block in blocks for g in range(4)]
    tops = {}

    def span_of(block):
        first = 2 * ROWS if part == "own" else block * BLOCK
        last = 2 * ROWS if part == "before" else block * BLOCK + SPAN
        return first, last, range(first, last, BLOCK)

    def place(block, g):
        columns = pl.ds(slot * 4 * HEAD + g * HEAD, HEAD)
        return slice(block * BLOCK, (block + 1) * BLOCK), columns

    def score(n, x):
        block, g = units[n]
        first, last, _ = span_of(block)
        span, seen = (slice(x - y, x - y + BLOCK) for y in (first, block * BLOCK))
        k = kv[slot, 0, x : x + BLOCK, :]
        s = lax.dot_general(
            q_ref[place(block, g)], k, (((1,), (1,)), ((), ())), preferred_element_type=jnp.float32
        )
        s = jnp.minimum(s, bias[block, :, seen])
        scores[n % 2, :, span] = s
        s = jnp.maximum(s[:, :HEAD], s[:, HEAD:])
        if x > first:
            s = jnp.maximum(s, tops[n])
        elif part == "before":
            s = jnp.maximum(s, state[2][head, block * 4 + g])
        tops[n] = jnp.max(s, axis=1, keepdims=True) if x + BLOCK == last else s

    def weigh(n, x):
        span = slice(x - span_of(units[n][0])[0], x - span_of(units[n][0])[0] + BLOCK)
        weights[n % 2, :, span] = scaled(scores[n % 2, :, span] - tops[n]).astype(jnp.bfloat16)

    def gather(n):
        block, g = units[n]
        unit = block * 4 + g
        first, last, _ = span_of(block)
        v = kv[slot, 1, first:last, :]
        v = jnp.concatenate([v, jnp.ones((last - first, HEAD), jnp.bfloat16)], axis=1)
        o = jnp.dot(weights[n % 2, :, : last - first], v, preferred_element_type=jnp.float32)
        o, total = o[:, :HEAD], o[:, HEAD:]
        if part == "own":
            state[0][head, unit] = o
            state[1][head, unit] = total
            state[2][head, unit] = jnp.broadcast_to(tops[n], (BLOCK, HEAD))
            return
        if part == "before":
            fade = scaled(state[2][head, unit] - tops[n])
            o += fade * state[0][head, unit]
            total += fade * state[1][head, unit]
        out[place(block, g)] = (o / total).astype(jnp.bfloat16)

    for x in span_of(units[0][0])[2]:
        score(0, x)
    for n in range(len(units)):
        now = list(span_of(units[n][0])[2])
        later = list(span_of(units[n + 1][0])[2]) if n + 1 < len(units) else []
        for i in range(max(len(now), len(later))):
            if i < len(later):
                score(n + 1, later[i])
            if i < len(now):
                weigh(n, now[i])
        gather(n)
        if n == 3 and between:
            between()


def fill_bias(start_ref, bias):
    shard = lax.axis_index("seqa") * lax.axis_size("seqb") + lax.axis_index("seqb")
    for block in range(2):
        starts = []
        for r in range(2):
            row = start_ref[pl.ds(block * 2 + r, 1), :] - shard * ROWS
            row = jnp.broadcast_to(row.astype(jnp.float32), (HEAD, HEAD))
            starts.append(row.T)
        start = jnp.concatenate(starts, axis=0)
        for t in range(SPAN // HEAD):
            q_place = lax.broadcasted_iota(jnp.int32, (BLOCK, HEAD), 0) + block * BLOCK
            k_place = lax.broadcasted_iota(jnp.int32, (BLOCK, HEAD), 1) + (
                t * HEAD + block * BLOCK - 2 * ROWS
            )
            seen = (
                (k_place <= q_place)
                & (k_place > q_place - 2 * ROWS)
                & (k_place.astype(jnp.float32) >= start)
            )
            bias[block, :, t * HEAD : (t + 1) * HEAD] = jnp.where(
                seen, jnp.float32(3e38), jnp.float32(-1e30)
            )


def head_columns(h):
    return pl.ds(pl.multiple_of(h * 4 * HEAD, 4 * HEAD), 4 * HEAD)


def kernel(
    chips, q_hbm, k_hbm, v_hbm, start_ref, o_hbm, kv_last,
    q_ref, kv, hop, bias, scores, weights, acc, total, top, out,
    kv_sem, q_sem, o_sem, pad_sem, far_send, far_recv, near_send, near_recv,
    hop_send, hop_recv,
):
    heads = kv.shape[0]
    at = places(chips)
    own, one, two = slice(1024, 1536), slice(512, 1024), slice(0, 512)
    rounds = range(len(ROUND))
    detour = sorted({h for h, _, _ in ROUND} - {SPLIT})
    cut = ROUND[-1][2]

    def load_kv(h, which):
        src = (k_hbm, v_hbm)[which]
        return pltpu.make_async_copy(
            src.at[:, pl.ds(h * HEAD, HEAD)], kv.at[h, which, own], kv_sem.at[h, which]
        )

    def load_q(h):
        columns = head_columns(h)
        return pltpu.make_async_copy(q_hbm.at[:, columns], q_ref.at[:, columns], q_sem.at[h])

    def store_o(h):
        columns = head_columns(h)
        return pltpu.make_async_copy(out.at[:, columns], o_hbm.at[:, columns], o_sem.at[h])

    def pad(h, which):
        src = (k_hbm, v_hbm)[which]
        return pltpu.make_async_copy(
            src.at[:, pl.ds(h * HEAD, HEAD)], kv.at[h, which, two], pad_sem.at[h, which]
        )

    def save():
        return pltpu.make_async_copy(kv.at[LAST, :, two], kv_last.at[:, two], o_sem.at[LAST])

    def sent(src, dst, sems, place):
        send, recv = sems
        return pltpu.make_async_remote_copy(
            src, dst, send, recv, device_id=at[place], device_id_type=MESH
        )

    def far(h):
        sems = far_send.at[h], far_recv.at[h]
        if h is SPLIT:
            src = kv.at[h, 1, own.start + cut : own.stop]
            return sent(src, kv.at[h, 1, two.start + cut : two.stop], sems, "after")
        return sent(kv.at[h, :, own], kv.at[h, :, two], sems, "after")

    def near(h, src):
        sems = near_send.at[h], near_recv.at[h]
        dst = kv_last.at[:, one] if h is LAST else kv.at[h, :, one]
        return sent(kv.at[h, :, src], dst, sems, "partner")

    def hops(stage, i):
        h, which, rows = ROUND[i]
        sems = hop_send.at[stage, i], hop_recv.at[stage, i]
        src = kv.at[h, which, own.start : own.start + rows]
        stops = src, hop.at[0, i, :rows], hop.at[1, i, :rows], kv.at[h, which, two.start : two.start + rows]
        place = "last_to" if stage == 2 else "down"
        return sent(stops[stage], stops[stage + 1], sems, place)

    def second(i):
        hops(0, i).wait_recv()
        hops(1, i).start()

    def third(i):
        hops(1, i).wait_recv()

        @pl.when(at["has_last_to"])
        def _():
            hops(2, i).start()

    order = [0, *detour, SPLIT, *(h for h in range(1, heads) if h not in (*detour, SPLIT))]
    for h in order:
        for which in range(2):
            load_kv(h, which).start()
    for h in range(heads - 1):
        load_q(h).start()

    barrier = pltpu.get_barrier_semaphore()

    def ready(name):
        pl.semaphore_signal(barrier, inc=1, device_id=at[name], device_id_type=MESH)

    ready("partner")
    ready("up")

    @pl.when(at["has_before"])
    def _():
        ready("before")
        ready("last_from")

    pl.semaphore_wait(barrier, at["peers"])

    for h in order:
        for which in range(2):
            load_kv(h, which).wait()
        for i in rounds:
            if ROUND[i][0] == h:
                hops(0, i).start()

        @pl.when(at["has_after"])
        def _():
            if h not in (*detour, SPLIT, LAST):
                far(h).start()

        @pl.when(at["core"] == 0)
        def _():
            near(h, own).start()

        @pl.when(jnp.logical_not(at["has_before"]))
        def _():
            for which in range(2):
                pad(h, which).start()

    @pl.when(at["has_after"])
    def _():
        far(SPLIT).start()
        far(LAST).start()

    fill_bias(start_ref, bias)
    state = (acc, total, top)

    def first_step(h, carry):
        load_q(h).wait()
        attend(h, h, q_ref, kv, bias, scores, weights, state, out, (0, 1), "own")

        @pl.when(h == heads - 3)
        def _():
            second(0)
            second(1)

        return carry

    lax.fori_loop(0, heads - 1, first_step, 0)

    def step(h, carry):
        @pl.when(h == 0)
        def _():
            second(2)
            second(3)

        for i in rounds:

            @pl.when(h == 2 + i // 2)
            def _():
                third(i)

        @pl.when(at["has_before"])
        def _():
            direct = True
            if isinstance(h, int):
                for i in rounds:
                    if ROUND[i][0] == SPLIT:
                        hops(2, i).wait_recv()
            for d in detour:
                direct &= h != d

                @pl.when(h == d)
                def _():
                    for i in rounds:
                        if ROUND[i][0] == d:
                            hops(2, i).wait_recv()

            @pl.when(direct)
            def _():
                far(h).wait_recv()

        @pl.when(jnp.logical_not(at["has_before"]))
        def _():
            for which in range(2):
                pad(h, which).wait()

        @pl.when(at["core"] == 1)
        def _():
            near(h, two).start()

        near(h, own).wait_recv()
        work = q_ref, kv, bias, scores, weights, state, out
        if not isinstance(h, int):
            attend(h, h, *work, (0, 1), "before")
        else:
            attend(h, h, *work, (0,), "before")

            @pl.when(at["has_before"])
            def _():
                far(LAST).wait_recv()

            @pl.when(jnp.logical_not(at["has_before"]))
            def _():
                for which in range(2):
                    pad(LAST, which).wait()

            @pl.when(at["core"] == 1)
            def _():
                near(LAST, two).start()

            save().start()
            attend(h, h, *work, (1,), "before")
        store_o(h).start()
        return carry

    lax.fori_loop(0, heads - 2, step, 0)
    step(SPLIT, 0)

    near(LAST, own).wait_recv()
    save().wait()
    for h in range(heads):
        if h != LAST:
            store_o(h).wait()
        near(h, own).wait_send()
        if h not in detour:

            @pl.when(at["has_after"])
            def _():
                far(h).wait_send()

    for i in rounds:
        hops(0, i).wait_send()
        hops(1, i).wait_send()

        @pl.when(at["has_last_to"])
        def _():
            hops(2, i).wait_send()


def finish(
    q_hbm, k_hbm, v_hbm, start_ref, first_hbm, kv_last, o_hbm,
    q_ref, kv, bias, scores, weights, out, kv_sem, q_sem, in_sem, o_sem,
):
    heads = k_hbm.shape[1] // HEAD
    columns = head_columns(LAST)
    loads = [
        pltpu.make_async_copy(kv_last, kv.at[0, :, : 2 * ROWS], kv_sem.at[0]),
        pltpu.make_async_copy(k_hbm.at[:, pl.ds(LAST * HEAD, HEAD)], kv.at[0, 0, 2 * ROWS :], kv_sem.at[1]),
        pltpu.make_async_copy(v_hbm.at[:, pl.ds(LAST * HEAD, HEAD)], kv.at[0, 1, 2 * ROWS :], kv_sem.at[2]),
        pltpu.make_async_copy(q_hbm.at[:, columns], q_ref, q_sem),
    ]
    takes = [
        pltpu.make_async_copy(first_hbm.at[:, head_columns(h)], out.at[h], in_sem.at[h])
        for h in range(heads - 1)
    ]
    stores = [
        pltpu.make_async_copy(out.at[h], o_hbm.at[:, head_columns(h)], o_sem.at[h])
        for h in range(heads - 1)
    ]
    halves = [
        pltpu.make_async_copy(
            out.at[LAST, pl.ds(block * BLOCK, BLOCK)],
            o_hbm.at[pl.ds(block * BLOCK, BLOCK), columns],
            o_sem.at[LAST + block],
        )
        for block in range(2)
    ]
    for copy in loads:
        copy.start()
    fill_bias(start_ref, bias)
    for copy in loads:
        copy.wait()
    for copy in takes:
        copy.start()

    def between():
        halves[0].start()
        for h in range(heads - 1):
            takes[h].wait()
            stores[h].start()

    attend(0, 0, q_ref, kv, bias, scores, weights, None, out.at[LAST], (0, 1), "all", between)
    halves[1].start()
    for copy in stores + halves:
        copy.wait()


def local(queries, keys, values, doc_start):
    heads = keys.shape[1] // HEAD
    chips = lax.axis_size("seqa") * lax.axis_size("seqb") // 2
    anywhere = pl.BlockSpec(memory_space=pl.ANY)
    held = pl.BlockSpec(memory_space=pltpu.VMEM)
    dma = pltpu.SemaphoreType.DMA
    starts = doc_start.reshape(ROWS // HEAD, HEAD)
    work = [
        pltpu.VMEM((2, BLOCK, SPAN), jnp.float32),
        pltpu.VMEM((2, BLOCK, SPAN), jnp.float32),
        pltpu.VMEM((2, BLOCK, SPAN), jnp.bfloat16),
    ]
    first, kv_last = pl.pallas_call(
        functools.partial(kernel, chips),
        out_shape=(
            jax.ShapeDtypeStruct(queries.shape, queries.dtype),
            jax.ShapeDtypeStruct((2, 2 * ROWS, HEAD), keys.dtype),
        ),
        in_specs=[anywhere] * 3 + [held],
        out_specs=(anywhere, anywhere),
        scratch_shapes=[
            pltpu.VMEM(queries.shape, jnp.bfloat16),
            pltpu.VMEM((heads, 2, 3 * ROWS, HEAD), jnp.bfloat16),
            pltpu.VMEM((2, len(ROUND), ROWS, HEAD), jnp.bfloat16),
            *work,
            *[pltpu.VMEM((heads - 1, 8, BLOCK, HEAD), jnp.float32)] * 3,
            pltpu.VMEM(queries.shape, jnp.bfloat16),
            dma((heads, 2)), dma((heads,)), dma((heads,)), dma((heads, 2)),
            dma((heads,)), dma((heads,)), dma((heads,)), dma((heads,)),
            dma((3, len(ROUND))), dma((3, len(ROUND))),
        ],
        compiler_params=pltpu.CompilerParams(
            collective_id=0, has_side_effects=True, vmem_limit_bytes=60 * 2**20
        ),
        name="attention",
    )(queries, keys, values, starts)
    return pl.pallas_call(
        finish,
        out_shape=jax.ShapeDtypeStruct(queries.shape, queries.dtype),
        in_specs=[anywhere] * 3 + [held] + [anywhere] * 2,
        out_specs=anywhere,
        scratch_shapes=[
            pltpu.VMEM((ROWS, 4 * HEAD), jnp.bfloat16),
            pltpu.VMEM((1, 2, 3 * ROWS, HEAD), jnp.bfloat16),
            *work,
            pltpu.VMEM((heads, ROWS, 4 * HEAD), jnp.bfloat16),
            dma((3,)), dma, dma((heads,)), dma((heads + 1,)),
        ],
        compiler_params=pltpu.CompilerParams(vmem_limit_bytes=60 * 2**20),
        name="finish",
    )(queries, keys, values, starts, first, kv_last)


def solution(mesh):
    shards = P(("seqa", "seqb"), None)
    return jax.shard_map(
        local,
        mesh=mesh,
        in_specs=(shards, shards, shards, P(("seqa", "seqb"))),
        out_specs=shards,
        check_vma=False,
    )
```
